512 devices in a mesh: ctx: 64 (over x_lo, z, core), tp: 8 (over y, x_hi).
Axes of the slice: x: 4 (x_hi: 2, x_lo: 2; x = x_hi * 2 + x_lo), y: 4, z: 16, core: 2. Of those that a mesh axis runs over, the one named last changes fastest.
Arguments:
- queries: bfloat16 [16384, 12288], P(('ctx', 'tp')), may hold values from -64 to 64
- keys: bfloat16 [16384, 1024], P(('ctx', 'tp')), may hold values from -4 to 4
- values: bfloat16 [16384, 1024], P(('ctx', 'tp')), may hold values from -6 to 6
- block_order: int32 [64], replicated, may hold values from 0 to 63, each once
Outputs:
- attended: bfloat16 [16384, 12288], P(('ctx', 'tp'))
The draws below stay inside these ranges and needn't reach their ends.
Inputs may be any that keep to these rules, and one draw needn't show every extreme that they name: A permutation: block r holds sequence span block_order[r] in its first 128 rows and span 2 * 64 - 1 - block_order[r] in its last 128 rows.
All inputs are finite; a program needn't handle non-finite values.
Results may differ from the reference program's by a relative error of at most 0.003.
Values may be sent and summed in bfloat16 or wider, within the bound.
A program may use at most 64 MiB of HBM per device.

```python
import math
import jax
import jax.numpy as jnp
from jax import lax

HD = 128
KV_HEADS = 8
HEADS = 96
PREV = 3
GROUP = 12
TOK_DEV = 256
SPAN = 128
BLOCKS = 64
TOKENS = 16384


def draw_keys(key, part):
    shape_keys = (TOKENS, KV_HEADS * HD)
    base = jnp.clip(jax.random.normal(jax.random.fold_in(key, 11), shape_keys, jnp.float32), -4.0, 4.0)
    return base.astype(jnp.bfloat16)


def draw_queries(key, part):
    shape_queries = (TOKENS, HEADS * HD)
    base = jnp.clip(3.0 * jax.random.normal(jax.random.fold_in(key, 21), shape_queries, jnp.float32), -12.0, 12.0)
    return base.astype(jnp.bfloat16)


def shard_levels(stream_key, dims, cuts, smallest, top_value):
    factor_of = 1.0
    for position, shards_of in cuts:
        draws = jax.random.uniform(jax.random.fold_in(jax.random.fold_in(stream_key, 6), position), (shards_of,), jnp.float32, smallest / len(cuts), top_value / len(cuts))
        factor_of = factor_of * jnp.repeat(jnp.exp(draws), dims[position] // shards_of).reshape((-1,) + (1,) * (len(dims) - 1 - position))
    return factor_of


def centred(stream_key, dims, scale, limit, cuts=(), held_as=jnp.bfloat16):
    level = shard_levels(stream_key, dims, cuts, -0.22, 0.18) if cuts else 1.0
    values = jax.random.normal(stream_key, dims, jnp.float32) * scale * level
    return jnp.minimum(jnp.maximum(values, -limit), limit).astype(held_as)


def setup_inputs(seed: int = 0) -> dict:
    key_of = jax.random.split(jax.random.key(seed), 5)
    queries = draw_queries(jax.random.fold_in(key_of[4], 71), 0)
    keys = draw_keys(jax.random.fold_in(key_of[4], 71), 0)
    values = centred(key_of[2], (TOKENS, KV_HEADS * HD), 1.0, 6.0, ((0, 512),))
    block_order = jax.random.permutation(key_of[3], BLOCKS).astype(jnp.int32)
    return {"queries": queries, "keys": keys, "values": values, "block_order": block_order}


MASKED_SCORE = -1e+30

def token_positions(block_order):
    row_ids = jnp.arange(TOKENS, dtype=jnp.int32)
    owner_block = row_ids // TOK_DEV
    within = row_ids % TOK_DEV
    leading = block_order[owner_block].astype(jnp.int32)
    early_pos = leading * SPAN + within
    late_pos = (2 * BLOCKS - 1 - leading) * SPAN + within - SPAN
    return jnp.where(within < SPAN, early_pos, late_pos).astype(jnp.int32)

def reference(queries, keys, values, block_order):
    token_pos = token_positions(block_order)
    key_blocks = keys.astype(jnp.float32).reshape(BLOCKS, TOK_DEV, KV_HEADS, HD)
    value_blocks = values.astype(jnp.float32).reshape(BLOCKS, TOK_DEV, KV_HEADS, HD)
    pos_blocks = token_pos.reshape(BLOCKS, TOK_DEV)
    query_rows = math.gcd(TOK_DEV, 64)
    grouped = queries.reshape(BLOCKS, TOK_DEV // query_rows, query_rows, KV_HEADS, GROUP, HD)
    query_pos = token_pos.reshape(BLOCKS, TOK_DEV // query_rows, query_rows)
    score_scale = 1.0 / math.sqrt(HD)

    def per_block(inputs_block):
        block_id, query_set, pos_set = inputs_block
        window = (block_id - jnp.arange(PREV + 1, dtype=jnp.int32)) % BLOCKS
        window_keys = key_blocks[window].reshape((PREV + 1) * TOK_DEV, KV_HEADS, HD)
        window_values = value_blocks[window].reshape((PREV + 1) * TOK_DEV, KV_HEADS, HD)
        window_pos = pos_blocks[window].reshape((PREV + 1) * TOK_DEV)

        def attend(inputs_pair):
            query_block, query_here = inputs_pair
            scores = jnp.einsum('tkgd,skd->tkgs', query_block.astype(jnp.float32), window_keys) * score_scale
            visible = window_pos[None, None, None, :] <= query_here[:, None, None, None]
            row_max = lax.optimization_barrier(jnp.max(jnp.where(visible, scores, MASKED_SCORE), axis=-1, keepdims=True))
            exp_scores = jnp.where(visible, jnp.exp(scores - row_max), 0.0)
            denominator = lax.optimization_barrier(jnp.sum(exp_scores, axis=-1))
            rounded = lax.optimization_barrier(exp_scores.astype(jnp.bfloat16))
            weights = rounded.astype(jnp.float32)
            numerator = jnp.einsum('tkgs,skd->tkgd', weights, window_values)
            result = numerator / denominator[..., None]
            return result.astype(jnp.bfloat16).reshape(query_rows, HEADS * HD)
        return lax.map(attend, (query_set, pos_set))
    block_ids = jnp.arange(BLOCKS, dtype=jnp.int32)
    attended = lax.map(per_block, (block_ids, grouped, query_pos))
    return attended.reshape(TOKENS, HEADS * HD)
```

```python
import functools
import math

import jax
import jax.numpy as jnp
from jax import lax
from jax.experimental import pallas as pl
from jax.experimental.pallas import tpu as pltpu
from jax.sharding import PartitionSpec as P

HD = 128
PREV = 3
MASKED_SCORE = -1e30
MESH = pl.DeviceIdType.MESH
ORDER = ((0, 0), (2, 0), (2, 1), (1, 1), (3, 1), (0, 1), (1, 0), (3, 0))


def pick(index, values):
    total = jnp.int32(0)
    for position, value in enumerate(values):
        if value:
            total = total + jnp.where(index == position, jnp.int32(value), jnp.int32(0))
    return total


def kernel(
    blocks, q_hbm, k_hbm, v_hbm, order_ref, out_hbm,
    q_buf, kv_buf, k_vm, v_vm, vext, o_buf,
    local_sem, kv_ss, kv_rs, q_ss, q_rs, f_ss, f_rs, o_ss, o_rs,
):
    ctx = lax.axis_index("ctx")
    tp = lax.axis_index("tp")
    rows = q_hbm.shape[0]
    width = q_buf.shape[2]
    group = width // HD
    y, xh = lax.div(tp, 2), lax.rem(tp, 2)

    def slot_of(dy, dx):
        return lax.rem(y + dy, 4) * 2 + lax.rem(xh + dx, 2)

    def lanes(slot, size):
        return pl.ds(pl.multiple_of(slot * size, size), size)

    ahead = [lax.rem(ctx + step, blocks) for step in range(1, PREV + 1)]
    behind = [lax.rem(ctx + blocks - step, blocks) for step in range(1, PREV + 1)]

    k_load = pltpu.make_async_copy(k_hbm, k_vm, local_sem.at[0])
    v_load = pltpu.make_async_copy(v_hbm, v_vm, local_sem.at[1])
    own_k = pltpu.make_async_copy(k_hbm.at[:, lanes(tp, HD)], kv_buf.at[0, tp, 0], local_sem.at[2])
    own_v = pltpu.make_async_copy(v_hbm.at[:, lanes(tp, HD)], kv_buf.at[0, tp, 1], local_sem.at[3])
    own_q = pltpu.make_async_copy(q_hbm.at[:, lanes(tp, width)], q_buf.at[tp], local_sem.at[4])
    for copy in (k_load, v_load, own_k, own_v, own_q):
        copy.start()

    barrier = pltpu.get_barrier_semaphore()
    for dy, dx in ORDER[1:]:
        pl.semaphore_signal(barrier, inc=1, device_id=(ctx, slot_of(dy, dx)), device_id_type=MESH)
    for other in behind:
        pl.semaphore_signal(barrier, inc=1, device_id=(other, tp), device_id_type=MESH)
    pl.semaphore_wait(barrier, len(ORDER) - 1 + PREV)

    def kv_copy(part, source, origin, peer):
        return pltpu.make_async_remote_copy(
            src_ref=source.at[:, lanes(peer, HD)],
            dst_ref=kv_buf.at[0, origin, part],
            send_sem=kv_ss.at[peer, part],
            recv_sem=kv_rs.at[origin, part],
            device_id=(ctx, peer),
            device_id_type=MESH,
        )

    def q_copy(origin, peer):
        return pltpu.make_async_remote_copy(
            src_ref=q_hbm.at[:, lanes(peer, width)],
            dst_ref=q_buf.at[origin],
            send_sem=q_ss.at[peer],
            recv_sem=q_rs.at[origin],
            device_id=(ctx, peer),
            device_id_type=MESH,
        )

    def forward(slot, step):
        return pltpu.make_async_remote_copy(
            src_ref=kv_buf.at[0, slot],
            dst_ref=kv_buf.at[step, slot],
            send_sem=f_ss.at[slot, step - 1],
            recv_sem=f_rs.at[slot, step - 1],
            device_id=(ahead[step - 1], tp),
            device_id_type=MESH,
        )

    def o_copy(origin, peer):
        return pltpu.make_async_remote_copy(
            src_ref=o_buf.at[peer],
            dst_ref=out_hbm.at[:, lanes(origin, width)],
            send_sem=o_ss.at[peer],
            recv_sem=o_rs.at[origin],
            device_id=(ctx, peer),
            device_id_type=MESH,
        )

    k_load.wait()
    v_load.wait()
    for dy, dx in ORDER[1:]:
        kv_copy(0, k_vm, tp, slot_of(dy, dx)).start()
        kv_copy(1, v_vm, tp, slot_of(dy, dx)).start()
    for dy, dx in ORDER[1:]:
        q_copy(tp, slot_of(dy, dx)).start()

    own_k.wait()
    own_v.wait()
    for dy, dx in ((0, 0), (1, 0), (3, 0), (0, 1), (1, 1), (3, 1), (2, 0), (2, 1)):
        slot = slot_of(dy, dx)
        if (dy, dx) != (0, 0):
            kv_copy(0, k_vm, slot, slot).wait_recv()
            kv_copy(1, v_vm, slot, slot).wait_recv()
        for step in range(1, PREV + 1):
            forward(slot, step).start()

    vext[:, :, HD:] = jnp.ones(vext.shape[:2] + (HD,), jnp.bfloat16)
    vext[0, :, :HD] = kv_buf[0, :, 1].reshape(8 * rows, HD)
    for step in range(1, PREV + 1):
        for slot in range(8):
            forward(slot, step).wait_recv()
        vext[step, :, :HD] = kv_buf[step, :, 1].reshape(8 * rows, HD)
    own_q.wait()

    here = order_ref[ctx]
    there = [order_ref[other] for other in behind]
    span = 4 * rows
    factor = math.log2(math.e) / math.sqrt(HD)

    def attend(slot, late):
        slots = 8 if late else 4
        count = slots * rows
        queries = jnp.concatenate([q_buf[slot, :, h * HD : (h + 1) * HD] for h in range(group)], axis=0)
        key_rows = kv_buf[:, :slots, 0].reshape((PREV + 1) * count, HD)
        scores = lax.dot_general(
            queries, key_rows, (((1,), (1,)), ((), ())), preferred_element_type=jnp.float32
        )
        first = slot * rows - (span if late else 0)
        own_row = lax.broadcasted_iota(jnp.int32, (rows, span), 0) + first
        own_col = lax.broadcasted_iota(jnp.int32, (rows, span), 1)
        causal = jnp.where(own_col <= own_row, 0.0, MASKED_SCORE).astype(jnp.float32)
        causal = jnp.concatenate([causal] * group, axis=0)
        pieces = []
        for step in range(PREV + 1):
            for half in range(slots // 4):
                start = step * count + half * span
                piece = scores[:, start : start + span]
                if half == (1 if late else 0):
                    if step == 0:
                        piece = piece + causal
                    else:
                        seen = there[step - 1] > here if late else there[step - 1] < here
                        piece = piece + jnp.where(seen, 0.0, MASKED_SCORE).astype(jnp.float32)
                pieces.append(piece)
        top = functools.reduce(jnp.maximum, pieces)
        top = jnp.max(top, axis=1, keepdims=True)
        weights = jnp.concatenate([jnp.exp2((piece - top) * factor).astype(jnp.bfloat16) for piece in pieces], axis=1)
        total = jnp.dot(
            weights, vext[:, :count].reshape((PREV + 1) * count, 2 * HD), preferred_element_type=jnp.float32
        )
        result = (total[:, :HD] / total[:, HD:]).astype(jnp.bfloat16)
        for h in range(group):
            o_buf[slot, :, h * HD : (h + 1) * HD] = result[h * rows : (h + 1) * rows]

    own_out = pltpu.make_async_copy(o_buf.at[tp], out_hbm.at[:, lanes(tp, width)], local_sem.at[5])

    def serve(turn, carry):
        slot = slot_of(pick(turn, [dy for dy, _ in ORDER]), pick(turn, [dx for _, dx in ORDER]))

        @pl.when(turn > 0)
        def _():
            q_copy(slot, slot).wait_recv()

        @pl.when(slot < 4)
        def _():
            attend(slot, False)

        @pl.when(slot >= 4)
        def _():
            attend(slot, True)

        @pl.when(turn > 0)
        def _():
            o_copy(tp, slot).start()

        @pl.when(turn == 0)
        def _():
            own_out.start()

        return carry

    lax.fori_loop(0, len(ORDER), serve, 0)

    own_out.wait()
    for dy, dx in ORDER[1:]:
        slot = slot_of(dy, dx)
        o_copy(slot, slot).wait_recv()
    for dy, dx in ORDER[1:]:
        slot = slot_of(dy, dx)
        o_copy(tp, slot).wait_send()
        q_copy(tp, slot).wait_send()
        kv_copy(0, k_vm, tp, slot).wait_send()
        kv_copy(1, v_vm, tp, slot).wait_send()
    for slot in range(8):
        for step in range(1, PREV + 1):
            forward(slot, step).wait_send()


def per_device(queries, keys, values, block_order):
    rows, width = queries.shape
    part = width // 8
    any_space = pl.BlockSpec(memory_space=pl.ANY)
    return pl.pallas_call(
        functools.partial(kernel, block_order.shape[0]),
        out_shape=jax.ShapeDtypeStruct(queries.shape, jnp.bfloat16),
        in_specs=[any_space, any_space, any_space, pl.BlockSpec(memory_space=pltpu.SMEM)],
        out_specs=any_space,
        scratch_shapes=[
            pltpu.VMEM((8, rows, part), jnp.bfloat16),
            pltpu.VMEM((PREV + 1, 8, 2, rows, HD), jnp.bfloat16),
            pltpu.VMEM(keys.shape, jnp.bfloat16),
            pltpu.VMEM(values.shape, jnp.bfloat16),
            pltpu.VMEM((PREV + 1, 8 * rows, 2 * HD), jnp.bfloat16),
            pltpu.VMEM((8, rows, part), jnp.bfloat16),
            pltpu.SemaphoreType.DMA((6,)),
            pltpu.SemaphoreType.DMA((8, 2)),
            pltpu.SemaphoreType.DMA((8, 2)),
            pltpu.SemaphoreType.DMA((8,)),
            pltpu.SemaphoreType.DMA((8,)),
            pltpu.SemaphoreType.DMA((8, PREV)),
            pltpu.SemaphoreType.DMA((8, PREV)),
            pltpu.SemaphoreType.DMA((8,)),
            pltpu.SemaphoreType.DMA((8,)),
        ],
        compiler_params=pltpu.CompilerParams(
            collective_id=0, has_side_effects=True, vmem_limit_bytes=48 * 2**20
        ),
    )(queries, keys, values, block_order)


def solution(mesh):
    return jax.shard_map(
        per_device,
        mesh=mesh,
        in_specs=(P(("ctx", "tp"), None), P(("ctx", "tp"), None), P(("ctx", "tp"), None), P()),
        out_specs=P(("ctx", "tp"), None),
        check_vma=False,
    )
```

```python
import functools
import math

import jax
import jax.numpy as jnp
from jax import lax
from jax.experimental import pallas as pl
from jax.experimental.pallas import tpu as pltpu
from jax.sharding import PartitionSpec as P

HD = 128
PREV = 3
MASKED_SCORE = -1e30
MESH = pl.DeviceIdType.MESH
ORDER = ((2, 1), (1, 1), (3, 1), (2, 0), (0, 1), (1, 0), (3, 0), (0, 0))
PEERS = ORDER[:-1]


def pick(index, values):
    total = jnp.int32(0)
    for position, value in enumerate(values):
        if value:
            total = total + jnp.where(index == position, jnp.int32(value), jnp.int32(0))
    return total


def kernel(
    blocks, q_hbm, k_hbm, v_hbm, order_hbm, out_ref,
    order_ref, q_buf, kv_buf, kv_own, vext, o_buf,
    order_sem, own_sem, load_sem, q_own_sem, o_own_sem,
    s_ss, s_rs, r_ss, q_ss, q_rs, o_ss, o_rs,
):
    ctx = lax.axis_index("ctx")
    tp = lax.axis_index("tp")
    planes = blocks // 2
    rows = q_hbm.shape[0]
    width = q_buf.shape[2]
    group = width // HD
    w, c = lax.div(ctx, 2), lax.rem(ctx, 2)
    y, xh = lax.div(tp, 2), lax.rem(tp, 2)

    def near(dy, dx):
        return lax.rem(y + dy, 4) * 2 + lax.rem(xh + dx, 2)

    def block_at(dw, core):
        return lax.rem(w + dw + planes, planes) * 2 + core

    def lanes(index, size):
        return pl.ds(pl.multiple_of(index * size, size), size)

    mate = (block_at(0, 1 - c), tp)

    loads = []
    for part, source in enumerate((k_hbm, v_hbm)):
        for h in range(8):
            loads.append(
                pltpu.make_async_copy(source.at[:, pl.ds(h * HD, HD)], kv_own.at[h, part], load_sem.at[h, part])
            )
    own_kv = [
        pltpu.make_async_copy(source.at[:, lanes(tp, HD)], kv_buf.at[0, tp, part], own_sem.at[part])
        for part, source in enumerate((k_hbm, v_hbm))
    ]
    own_q = pltpu.make_async_copy(q_hbm.at[:, lanes(tp, width)], q_buf.at[tp], q_own_sem)
    order_load = pltpu.make_async_copy(order_hbm, order_ref, order_sem)
    for copy in (*loads, *own_kv, own_q, order_load):
        copy.start()

    barrier = pltpu.get_barrier_semaphore()

    def greet(block, slot):
        pl.semaphore_signal(barrier, inc=1, device_id=(block, slot), device_id_type=MESH)

    for dy, dx in ORDER:
        greet(block_at(-1, c), near(dy, dx))

    @pl.when(c == 0)
    def _():
        for dy, dx in ORDER:
            greet(block_at(-2, 1), near(dy, dx))

    for dy, dx in PEERS:
        greet(ctx, near(dy, dx))
    greet(*mate)
    pl.semaphore_wait(barrier, 16 + 8 * c)

    def slice_copy(dw, slot):
        return pltpu.make_async_remote_copy(
            src_ref=kv_own.at[slot],
            dst_ref=kv_buf.at[(0, 2, 3)[dw], tp],
            send_sem=s_ss.at[dw, slot],
            recv_sem=s_rs.at[(0, 2, 3)[dw], tp],
            device_id=(block_at(dw, 0 if dw == 2 else c), slot),
            device_id_type=MESH,
        )

    def relay(offset, landing, slot):
        return pltpu.make_async_remote_copy(
            src_ref=kv_buf.at[offset, slot],
            dst_ref=kv_buf.at[landing, slot],
            send_sem=r_ss.at[offset // 2, slot],
            recv_sem=s_rs.at[landing, slot],
            device_id=mate,
            device_id_type=MESH,
        )

    def arrived(offset, slot):
        relay(0, offset, slot).wait_recv()

    def q_copy(origin, slot):
        return pltpu.make_async_remote_copy(
            src_ref=q_hbm.at[:, lanes(slot, width)],
            dst_ref=q_buf.at[origin],
            send_sem=q_ss.at[slot],
            recv_sem=q_rs.at[origin],
            device_id=(ctx, slot),
            device_id_type=MESH,
        )

    def o_copy(origin, slot):
        return pltpu.make_async_remote_copy(
            src_ref=o_buf.at[slot],
            dst_ref=out_ref.at[:, lanes(origin, width)],
            send_sem=o_ss.at[slot],
            recv_sem=o_rs.at[origin],
            device_id=(ctx, slot),
            device_id_type=MESH,
        )

    for copy in loads:
        copy.wait()
    for dy, dx in ORDER:
        slice_copy(1, near(dy, dx)).start()

    @pl.when(c == 1)
    def _():
        for dy, dx in ORDER:
            slice_copy(2, near(dy, dx)).start()

    for dy, dx in PEERS:
        slice_copy(0, near(dy, dx)).start()
    for dy, dx in PEERS:
        q_copy(tp, near(dy, dx)).start()

    for copy in own_kv:
        copy.wait()
    for dy, dx in reversed(PEERS):
        arrived(0, near(dy, dx))

        @pl.when(c == 0)
        def _(slot=near(dy, dx)):
            relay(0, 1, slot).start()

    @pl.when(c == 0)
    def _():
        relay(0, 1, tp).start()

    for dy, dx in reversed(ORDER):
        arrived(2, near(dy, dx))

        @pl.when(c == 0)
        def _(slot=near(dy, dx)):
            relay(2, 3, slot).start()

        @pl.when(c == 1)
        def _(slot=near(dy, dx)):
            relay(2, 1, slot).start()

    vext[:, :, HD:] = jnp.ones((PREV + 1, 8 * rows, HD), jnp.bfloat16)
    for offset in (0, 2, 1, 3):
        if offset % 2:
            for slot in range(8):
                arrived(offset, slot)
        vext[offset, :, :HD] = kv_buf[offset, :, 1].reshape(8 * rows, HD)
    own_q.wait()
    order_load.wait()

    span = 4 * rows
    factor = math.log2(math.e) / math.sqrt(HD)

    here = order_ref[ctx]
    there = [order_ref[lax.rem(ctx + blocks - step, blocks)] for step in range(1, PREV + 1)]

    def attend(slot, late):
        slots = 8 if late else 4
        count = slots * rows
        queries = jnp.concatenate([q_buf[slot, :, h * HD : (h + 1) * HD] for h in range(group)], axis=0)
        key_rows = kv_buf[:, :slots, 0].reshape((PREV + 1) * count, HD)
        scores = lax.dot_general(
            queries, key_rows, (((1,), (1,)), ((), ())), preferred_element_type=jnp.float32
        )
        first = slot * rows - (span if late else 0)
        own_row = lax.broadcasted_iota(jnp.int32, (rows, span), 0) + first
        own_col = lax.broadcasted_iota(jnp.int32, (rows, span), 1)
        causal = jnp.where(own_col <= own_row, 0.0, MASKED_SCORE).astype(jnp.float32)
        causal = jnp.concatenate([causal] * group, axis=0)
        pieces = []
        for step in range(PREV + 1):
            for half in range(count // span):
                start = step * count + half * span
                piece = scores[:, start : start + span]
                if half == (1 if late else 0):
                    if step == 0:
                        piece = piece + causal
                    else:
                        seen = there[step - 1] > here if late else there[step - 1] < here
                        piece = piece + jnp.where(seen, 0.0, MASKED_SCORE).astype(jnp.float32)
                pieces.append(piece)
        top = functools.reduce(jnp.maximum, pieces)
        top = jnp.max(top, axis=1, keepdims=True)
        weights = jnp.concatenate([jnp.exp2((piece - top) * factor).astype(jnp.bfloat16) for piece in pieces], axis=1)
        total = jnp.dot(
            weights, vext[:, :count].reshape((PREV + 1) * count, 2 * HD), preferred_element_type=jnp.float32
        )
        result = (total[:, :HD] / total[:, HD:]).astype(jnp.bfloat16)
        for h in range(group):
            o_buf[slot, :, h * HD : (h + 1) * HD] = result[h * rows : (h + 1) * rows]

    own_out = pltpu.make_async_copy(o_buf.at[tp], out_ref.at[:, lanes(tp, width)], o_own_sem)

    def serve(turn, carry):
        slot = near(pick(turn, [dy for dy, _ in ORDER]), pick(turn, [dx for _, dx in ORDER]))

        @pl.when(turn < len(PEERS))
        def _():
            q_copy(slot, slot).wait_recv()

        @pl.when(slot < 4)
        def _():
            attend(slot, False)

        @pl.when(slot >= 4)
        def _():
            attend(slot, True)

        @pl.when(turn < len(PEERS))
        def _():
            o_copy(tp, slot).start()

        return carry

    lax.fori_loop(0, len(ORDER), serve, 0)
    own_out.start()

    for dy, dx in PEERS:
        slot = near(dy, dx)
        q_copy(tp, slot).wait_send()
        slice_copy(0, slot).wait_send()
    for dy, dx in ORDER:
        slot = near(dy, dx)
        slice_copy(1, slot).wait_send()
        relay(2, 1, slot).wait_send()

    @pl.when(c == 0)
    def _():
        for dy, dx in ORDER:
            relay(0, 1, near(dy, dx)).wait_send()

    @pl.when(c == 1)
    def _():
        for dy, dx in ORDER:
            slice_copy(2, near(dy, dx)).wait_send()

    own_out.wait()
    for dy, dx in PEERS:
        slot = near(dy, dx)
        o_copy(tp, slot).wait_send()
        o_copy(slot, slot).wait_recv()


def per_device(queries, keys, values, block_order):
    rows, width = queries.shape
    part = width // 8
    hbm = pl.BlockSpec(memory_space=pl.ANY)
    window = PREV + 1
    dma = pltpu.SemaphoreType.DMA
    return pl.pallas_call(
        functools.partial(kernel, block_order.shape[0]),
        out_shape=jax.ShapeDtypeStruct(queries.shape, jnp.bfloat16),
        in_specs=[hbm, hbm, hbm, hbm],
        out_specs=hbm,
        scratch_shapes=[
            pltpu.SMEM(block_order.shape, jnp.int32),
            pltpu.VMEM((8, rows, part), jnp.bfloat16),
            pltpu.VMEM((window, 8, 2, rows, HD), jnp.bfloat16),
            pltpu.VMEM((8, 2, rows, HD), jnp.bfloat16),
            pltpu.VMEM((window, 8 * rows, 2 * HD), jnp.bfloat16),
            pltpu.VMEM((8, rows, part), jnp.bfloat16),
            dma, dma((2,)), dma((8, 2)), dma, dma,
            dma((3, 8)), dma((window, 8)), dma((2, 8)),
            dma((8,)), dma((8,)), dma((8,)), dma((8,)),
        ],
        compiler_params=pltpu.CompilerParams(
            collective_id=0, has_side_effects=True, vmem_limit_bytes=65500000
        ),
    )(queries, keys, values, block_order)


def solution(mesh):
    return jax.shard_map(
        per_device,
        mesh=mesh,
        in_specs=(P(("ctx", "tp"), None), P(("ctx", "tp"), None), P(("ctx", "tp"), None), P()),
        out_specs=P(("ctx", "tp"), None),
        check_vma=False,
    )
```

```python
import functools
import math

import jax
import jax.numpy as jnp
from jax import lax
from jax.experimental import pallas as pl
from jax.experimental.pallas import tpu as pltpu
from jax.sharding import PartitionSpec as P

HD = 128
PREV = 3
MASKED_SCORE = -1e30
MESH = pl.DeviceIdType.MESH
ORDER = ((2, 1), (1, 1), (3, 1), (2, 0), (0, 1), (1, 0), (3, 0), (0, 0))
PEERS = ORDER[:-1]


def pick(index, values):
    total = jnp.int32(0)
    for position, value in enumerate(values):
        if value:
            total = total + jnp.where(index == position, jnp.int32(value), jnp.int32(0))
    return total


def kernel(
    blocks, q_hbm, k_hbm, v_hbm, order_hbm, out_ref,
    order_ref, q_buf, kv_buf, kv_own, vext, o_buf,
    order_sem, own_sem, load_sem, q_own_sem, o_own_sem,
    s_ss, s_rs, r_ss, q_ss, q_rs, o_ss, o_rs,
):
    ctx = lax.axis_index("ctx")
    tp = lax.axis_index("tp")
    planes = blocks // 2
    rows = q_hbm.shape[0]
    width = q_buf.shape[2]
    group = width // HD
    w, c = lax.div(ctx, 2), lax.rem(ctx, 2)
    y, xh = lax.div(tp, 2), lax.rem(tp, 2)

    def near(dy, dx):
        return lax.rem(y + dy, 4) * 2 + lax.rem(xh + dx, 2)

    def block_at(dw, core):
        return lax.rem(w + dw + planes, planes) * 2 + core

    def lanes(index, size):
        return pl.ds(pl.multiple_of(index * size, size), size)

    mate = (block_at(0, 1 - c), tp)

    loads = []
    for part, source in enumerate((k_hbm, v_hbm)):
        for h in range(8):
            loads.append(
                pltpu.make_async_copy(source.at[:, pl.ds(h * HD, HD)], kv_own.at[h, part], load_sem.at[h, part])
            )
    own_kv = [
        pltpu.make_async_copy(source.at[:, lanes(tp, HD)], kv_buf.at[0, tp, part], own_sem.at[part])
        for part, source in enumerate((k_hbm, v_hbm))
    ]
    own_q = pltpu.make_async_copy(q_hbm.at[:, lanes(tp, width)], q_buf.at[tp], q_own_sem)
    order_load = pltpu.make_async_copy(order_hbm, order_ref, order_sem)
    for copy in (*loads, *own_kv, own_q, order_load):
        copy.start()

    barrier = pltpu.get_barrier_semaphore()

    def greet(block, slot):
        pl.semaphore_signal(barrier, inc=1, device_id=(block, slot), device_id_type=MESH)

    for dy, dx in ORDER:
        greet(block_at(-1, c), near(dy, dx))

    @pl.when(c == 0)
    def _():
        greet(block_at(-1, 1), tp)

    for dy, dx in PEERS:
        greet(ctx, near(dy, dx))
    greet(*mate)
    pl.semaphore_wait(barrier, 16 + c)

    def slice_copy(dw, slot):
        return pltpu.make_async_remote_copy(
            src_ref=kv_own.at[slot],
            dst_ref=kv_buf.at[2 * dw, tp],
            send_sem=s_ss.at[dw, slot],
            recv_sem=s_rs.at[2 * dw, tp],
            device_id=(block_at(dw, c), slot),
            device_id_type=MESH,
        )

    def onward(slot):
        return pltpu.make_async_remote_copy(
            src_ref=kv_buf.at[2, slot],
            dst_ref=kv_buf.at[3, slot],
            send_sem=s_ss.at[2, slot],
            recv_sem=s_rs.at[3, slot],
            device_id=(block_at(1, 0), tp),
            device_id_type=MESH,
        )

    def relay(offset, landing, slot):
        return pltpu.make_async_remote_copy(
            src_ref=kv_buf.at[offset, slot],
            dst_ref=kv_buf.at[landing, slot],
            send_sem=r_ss.at[offset // 2, slot],
            recv_sem=s_rs.at[landing, slot],
            device_id=mate,
            device_id_type=MESH,
        )

    def arrived(offset, slot):
        relay(0, offset, slot).wait_recv()

    def q_copy(origin, slot):
        return pltpu.make_async_remote_copy(
            src_ref=q_hbm.at[:, lanes(slot, width)],
            dst_ref=q_buf.at[origin],
            send_sem=q_ss.at[slot],
            recv_sem=q_rs.at[origin],
            device_id=(ctx, slot),
            device_id_type=MESH,
        )

    def o_copy(origin, slot):
        return pltpu.make_async_remote_copy(
            src_ref=o_buf.at[slot],
            dst_ref=out_ref.at[:, lanes(origin, width)],
            send_sem=o_ss.at[slot],
            recv_sem=o_rs.at[origin],
            device_id=(ctx, slot),
            device_id_type=MESH,
        )

    for copy in loads:
        copy.wait()
    for dy, dx in ORDER:
        slice_copy(1, near(dy, dx)).start()

    for dy, dx in PEERS:
        slice_copy(0, near(dy, dx)).start()
    for dy, dx in PEERS:
        q_copy(tp, near(dy, dx)).start()

    for copy in own_kv:
        copy.wait()
    for dy, dx in reversed(PEERS):
        arrived(0, near(dy, dx))

        @pl.when(c == 0)
        def _(slot=near(dy, dx)):
            relay(0, 1, slot).start()

    @pl.when(c == 0)
    def _():
        relay(0, 1, tp).start()

    for dy, dx in reversed(ORDER):
        arrived(2, near(dy, dx))

        @pl.when(c == 0)
        def _(slot=near(dy, dx)):
            relay(2, 3, slot).start()

        @pl.when(c == 1)
        def _(slot=near(dy, dx)):
            onward(slot).start()
            relay(2, 1, slot).start()

    vext[:, :, HD:] = jnp.ones((PREV + 1, 8 * rows, HD), jnp.bfloat16)
    for offset in (0, 2, 1, 3):
        if offset % 2:
            for slot in range(8):
                arrived(offset, slot)
        vext[offset, :, :HD] = kv_buf[offset, :, 1].reshape(8 * rows, HD)
    own_q.wait()
    order_load.wait()

    span = 4 * rows
    factor = math.log2(math.e) / math.sqrt(HD)

    here = order_ref[ctx]
    there = [order_ref[lax.rem(ctx + blocks - step, blocks)] for step in range(1, PREV + 1)]

    def attend(slot, late):
        slots = 8 if late else 4
        count = slots * rows
        queries = jnp.concatenate([q_buf[slot, :, h * HD : (h + 1) * HD] for h in range(group)], axis=0)
        key_rows = kv_buf[:, :slots, 0].reshape((PREV + 1) * count, HD)
        scores = lax.dot_general(
            queries, key_rows, (((1,), (1,)), ((), ())), preferred_element_type=jnp.float32
        )
        first = slot * rows - (span if late else 0)
        own_row = lax.broadcasted_iota(jnp.int32, (rows, span), 0) + first
        own_col = lax.broadcasted_iota(jnp.int32, (rows, span), 1)
        causal = jnp.where(own_col <= own_row, 0.0, MASKED_SCORE).astype(jnp.float32)
        causal = jnp.concatenate([causal] * group, axis=0)
        pieces = []
        for step in range(PREV + 1):
            for half in range(count // span):
                start = step * count + half * span
                piece = scores[:, start : start + span]
                if half == (1 if late else 0):
                    if step == 0:
                        piece = piece + causal
                    else:
                        seen = there[step - 1] > here if late else there[step - 1] < here
                        piece = piece + jnp.where(seen, 0.0, MASKED_SCORE).astype(jnp.float32)
                pieces.append(piece)
        top = functools.reduce(jnp.maximum, pieces)
        top = jnp.max(top, axis=1, keepdims=True)
        weights = jnp.concatenate([jnp.exp2((piece - top) * factor).astype(jnp.bfloat16) for piece in pieces], axis=1)
        total = jnp.dot(
            weights, vext[:, :count].reshape((PREV + 1) * count, 2 * HD), preferred_element_type=jnp.float32
        )
        result = (total[:, :HD] / total[:, HD:]).astype(jnp.bfloat16)
        for h in range(group):
            o_buf[slot, :, h * HD : (h + 1) * HD] = result[h * rows : (h + 1) * rows]

    own_out = pltpu.make_async_copy(o_buf.at[tp], out_ref.at[:, lanes(tp, width)], o_own_sem)

    def serve(turn, carry):
        slot = near(pick(turn, [dy for dy, _ in ORDER]), pick(turn, [dx for _, dx in ORDER]))

        @pl.when(turn < len(PEERS))
        def _():
            q_copy(slot, slot).wait_recv()

        @pl.when(slot < 4)
        def _():
            attend(slot, False)

        @pl.when(slot >= 4)
        def _():
            attend(slot, True)

        @pl.when(turn < len(PEERS))
        def _():
            o_copy(tp, slot).start()

        return carry

    lax.fori_loop(0, len(ORDER), serve, 0)
    own_out.start()

    for dy, dx in PEERS:
        slot = near(dy, dx)
        q_copy(tp, slot).wait_send()
        slice_copy(0, slot).wait_send()
    for dy, dx in ORDER:
        slot = near(dy, dx)
        slice_copy(1, slot).wait_send()
        relay(2, 1, slot).wait_send()

    @pl.when(c == 0)
    def _():
        for dy, dx in ORDER:
            relay(0, 1, near(dy, dx)).wait_send()

    @pl.when(c == 1)
    def _():
        for dy, dx in ORDER:
            onward(near(dy, dx)).wait_send()

    own_out.wait()
    for dy, dx in PEERS:
        slot = near(dy, dx)
        o_copy(tp, slot).wait_send()
        o_copy(slot, slot).wait_recv()


def per_device(queries, keys, values, block_order):
    rows, width = queries.shape
    part = width // 8
    hbm = pl.BlockSpec(memory_space=pl.ANY)
    window = PREV + 1
    dma = pltpu.SemaphoreType.DMA
    return pl.pallas_call(
        functools.partial(kernel, block_order.shape[0]),
        out_shape=jax.ShapeDtypeStruct(queries.shape, jnp.bfloat16),
        in_specs=[hbm, hbm, hbm, hbm],
        out_specs=hbm,
        scratch_shapes=[
            pltpu.SMEM(block_order.shape, jnp.int32),
            pltpu.VMEM((8, rows, part), jnp.bfloat16),
            pltpu.VMEM((window, 8, 2, rows, HD), jnp.bfloat16),
            pltpu.VMEM((8, 2, rows, HD), jnp.bfloat16),
            pltpu.VMEM((window, 8 * rows, 2 * HD), jnp.bfloat16),
            pltpu.VMEM((8, rows, part), jnp.bfloat16),
            dma, dma((2,)), dma((8, 2)), dma, dma,
            dma((3, 8)), dma((window, 8)), dma((2, 8)),
            dma((8,)), dma((8,)), dma((8,)), dma((8,)),
        ],
        compiler_params=pltpu.CompilerParams(
            collective_id=0, has_side_effects=True, vmem_limit_bytes=50331648
        ),
    )(*[pltpu.with_memory_space_constraint(a, pltpu.HBM) for a in (queries, keys, values, block_order)])


def solution(mesh):
    return jax.shard_map(
        per_device,
        mesh=mesh,
        in_specs=(P(("ctx", "tp"), None), P(("ctx", "tp"), None), P(("ctx", "tp"), None), P()),
        out_specs=P(("ctx", "tp"), None),
        check_vma=False,
    )
```

```python
import functools
import math

import jax
import jax.numpy as jnp
from jax import lax
from jax.experimental import pallas as pl
from jax.experimental.pallas import tpu as pltpu
from jax.sharding import PartitionSpec as P

HD = 128
PREV = 3
MASKED_SCORE = -1e30
MESH = pl.DeviceIdType.MESH
ORDER = ((2, 1), (1, 1), (3, 1), (2, 0), (0, 1), (1, 0), (3, 0), (0, 0))
PEERS = ORDER[:-1]
PARTS = ((0, 1), (2, 3))


def pick(index, values):
    total = jnp.int32(0)
    for position, value in enumerate(values):
        if value:
            total = total + jnp.where(index == position, jnp.int32(value), jnp.int32(0))
    return total


def kernel(
    blocks, q_hbm, k_hbm, v_hbm, order_hbm, out_ref,
    order_ref, q_buf, kv_buf, kv_own, vext, o_buf,
    clear_sem, order_sem, own_sem, load_sem, q_own_sem, o_own_sem,
    s_ss, s_rs, r_ss, q_ss, q_rs, o_ss, o_rs,
):
    ctx = lax.axis_index("ctx")
    tp = lax.axis_index("tp")
    planes = blocks // 2
    rows = q_hbm.shape[0]
    width = q_buf.shape[2]
    group = width // HD
    w, c = lax.div(ctx, 2), lax.rem(ctx, 2)
    y, xh = lax.div(tp, 2), lax.rem(tp, 2)

    def near(dy, dx):
        return lax.rem(y + dy, 4) * 2 + lax.rem(xh + dx, 2)

    def block_at(dw, core):
        return lax.rem(w + dw + planes, planes) * 2 + core

    def lanes(index, size):
        return pl.ds(pl.multiple_of(index * size, size), size)

    mate = (block_at(0, 1 - c), tp)

    loads = []
    for part, source in enumerate((k_hbm, v_hbm)):
        for h in range(8):
            loads.append(
                pltpu.make_async_copy(source.at[:, pl.ds(h * HD, HD)], kv_own.at[h, part], load_sem.at[h, part])
            )
    own_kv = [
        pltpu.make_async_copy(source.at[:, lanes(tp, HD)], kv_buf.at[0, tp, part], own_sem.at[part])
        for part, source in enumerate((k_hbm, v_hbm))
    ]
    own_q = pltpu.make_async_copy(q_hbm.at[:, lanes(tp, width)], q_buf.at[tp], q_own_sem)
    order_load = pltpu.make_async_copy(order_hbm, order_ref, order_sem)
    for copy in (*loads, *own_kv, own_q, order_load):
        copy.start()

    barrier = pltpu.get_barrier_semaphore()

    def greet(block, slot):
        pl.semaphore_signal(barrier, inc=1, device_id=(block, slot), device_id_type=MESH)

    for dy, dx in ORDER:
        greet(block_at(-1, c), near(dy, dx))

    @pl.when(c == 0)
    def _():
        greet(block_at(-1, 1), tp)

    last = lax.rem(w, planes // 2) == planes // 2 - 1

    @pl.when(jnp.logical_not(last))
    def _():
        for dy, dx in PEERS:
            greet(ctx, near(dy, dx))

    greet(*mate)
    pl.semaphore_wait(barrier, jnp.where(last, 9 + c, 16 + c))

    @pl.when(lax.rem(w + 1, planes // 2) == planes // 2 - 1)
    def _():
        pl.semaphore_signal(clear_sem, inc=1, device_id=(block_at(1, c), tp), device_id_type=MESH)

    def slice_copy(dw, slot):
        return pltpu.make_async_remote_copy(
            src_ref=kv_own.at[slot],
            dst_ref=kv_buf.at[2 * dw, tp],
            send_sem=s_ss.at[dw, slot],
            recv_sem=s_rs.at[2 * dw, tp],
            device_id=(block_at(dw, c), slot),
            device_id_type=MESH,
        )

    def onward(slot):
        return pltpu.make_async_remote_copy(
            src_ref=kv_buf.at[2, slot],
            dst_ref=kv_buf.at[3, slot],
            send_sem=s_ss.at[2, slot],
            recv_sem=s_rs.at[3, slot],
            device_id=(block_at(1, 0), tp),
            device_id_type=MESH,
        )

    def relay(offset, landing, slot):
        return pltpu.make_async_remote_copy(
            src_ref=kv_buf.at[offset, slot],
            dst_ref=kv_buf.at[landing, slot],
            send_sem=r_ss.at[offset // 2, slot],
            recv_sem=s_rs.at[landing, slot],
            device_id=mate,
            device_id_type=MESH,
        )

    def arrived(offset, slot):
        relay(0, offset, slot).wait_recv()

    def q_copy(origin, slot):
        return pltpu.make_async_remote_copy(
            src_ref=q_hbm.at[:, lanes(slot, width)],
            dst_ref=q_buf.at[origin],
            send_sem=q_ss.at[slot],
            recv_sem=q_rs.at[origin],
            device_id=(ctx, slot),
            device_id_type=MESH,
        )

    def o_copy(origin, slot):
        return pltpu.make_async_remote_copy(
            src_ref=o_buf.at[slot],
            dst_ref=out_ref.at[:, lanes(origin, width)],
            send_sem=o_ss.at[slot],
            recv_sem=o_rs.at[origin],
            device_id=(ctx, slot),
            device_id_type=MESH,
        )

    for copy in loads:
        copy.wait()
    for dy, dx in ORDER:
        slice_copy(1, near(dy, dx)).start()

    @pl.when(last)
    def _():
        pl.semaphore_wait(clear_sem, 1)

    for dy, dx in PEERS:
        slice_copy(0, near(dy, dx)).start()
    for dy, dx in PEERS:
        q_copy(tp, near(dy, dx)).start()

    for copy in own_kv:
        copy.wait()
    for dy, dx in reversed(PEERS):
        arrived(0, near(dy, dx))

        @pl.when(c == 0)
        def _(slot=near(dy, dx)):
            relay(0, 1, slot).start()

    @pl.when(c == 0)
    def _():
        relay(0, 1, tp).start()

    for dy, dx in reversed(ORDER):
        arrived(2, near(dy, dx))

        @pl.when(c == 0)
        def _(slot=near(dy, dx)):
            relay(2, 3, slot).start()

        @pl.when(c == 1)
        def _(slot=near(dy, dx)):
            onward(slot).start()
            relay(2, 1, slot).start()

    vext[:, :, HD:] = jnp.ones((PREV + 1, 8 * rows, HD), jnp.bfloat16)
    for offset in (0, 2, 1, 3):
        if offset % 2:
            for slot in range(8):
                arrived(offset, slot)
        vext[offset, :, :HD] = kv_buf[offset, :, 1].reshape(8 * rows, HD)
    own_q.wait()
    order_load.wait()

    span = 4 * rows
    factor = math.log2(math.e) / math.sqrt(HD)

    here = order_ref[ctx]
    there = [order_ref[lax.rem(ctx + blocks - step, blocks)] for step in range(1, PREV + 1)]

    def attend(slot, late):
        slots = 8 if late else 4
        count = slots * rows
        queries = jnp.concatenate([q_buf[slot, :, h * HD : (h + 1) * HD] for h in range(group)], axis=0)
        first = slot * rows - (span if late else 0)
        own_row = lax.broadcasted_iota(jnp.int32, (rows, span), 0) + first
        own_col = lax.broadcasted_iota(jnp.int32, (rows, span), 1)
        causal = jnp.where(own_col <= own_row, 0.0, MASKED_SCORE).astype(jnp.float32)
        causal = jnp.concatenate([causal] * group, axis=0)

        def scored(offsets):
            key_rows = kv_buf[offsets[0] : offsets[-1] + 1, :slots, 0].reshape(len(offsets) * count, HD)
            scores = lax.dot_general(
                queries, key_rows, (((1,), (1,)), ((), ())), preferred_element_type=jnp.float32
            )
            pieces = []
            for position, offset in enumerate(offsets):
                for half in range(slots // 4):
                    start = position * count + half * span
                    piece = scores[:, start : start + span]
                    if half == (1 if late else 0):
                        if offset == 0:
                            piece = piece + causal
                        else:
                            seen = there[offset - 1] > here if late else there[offset - 1] < here
                            piece = piece + jnp.where(seen, 0.0, MASKED_SCORE).astype(jnp.float32)
                    pieces.append(piece)
            return pieces

        total, top = None, None
        parts = [scored(offsets) for offsets in PARTS]
        for offsets, pieces in zip(PARTS, parts):
            best = jnp.max(functools.reduce(jnp.maximum, pieces), axis=1, keepdims=True)
            if top is not None:
                best = jnp.maximum(best, top)
            weights = jnp.concatenate(
                [jnp.exp2((piece - best) * factor).astype(jnp.bfloat16) for piece in pieces], axis=1
            )
            sums = jnp.dot(
                weights,
                vext[offsets[0] : offsets[-1] + 1, :count].reshape(len(offsets) * count, 2 * HD),
                preferred_element_type=jnp.float32,
            )
            total = sums if total is None else total * jnp.exp2((top - best) * factor) + sums
            top = best
        result = (total[:, :HD] / total[:, HD:]).astype(jnp.bfloat16)
        for h in range(group):
            o_buf[slot, :, h * HD : (h + 1) * HD] = result[h * rows : (h + 1) * rows]

    own_out = pltpu.make_async_copy(o_buf.at[tp], out_ref.at[:, lanes(tp, width)], o_own_sem)

    def serve(turn, carry):
        slot = near(pick(turn, [dy for dy, _ in ORDER]), pick(turn, [dx for _, dx in ORDER]))

        @pl.when(turn < len(PEERS))
        def _():
            q_copy(slot, slot).wait_recv()

        @pl.when(slot < 4)
        def _():
            attend(slot, False)

        @pl.when(slot >= 4)
        def _():
            attend(slot, True)

        @pl.when(turn < len(PEERS))
        def _():
            o_copy(tp, slot).start()

        return carry

    lax.fori_loop(0, len(ORDER), serve, 0)
    own_out.start()

    for dy, dx in PEERS:
        slot = near(dy, dx)
        q_copy(tp, slot).wait_send()
        slice_copy(0, slot).wait_send()
    for dy, dx in ORDER:
        slot = near(dy, dx)
        slice_copy(1, slot).wait_send()
        relay(2, 1, slot).wait_send()

    @pl.when(c == 0)
    def _():
        for dy, dx in ORDER:
            relay(0, 1, near(dy, dx)).wait_send()

    @pl.when(c == 1)
    def _():
        for dy, dx in ORDER:
            onward(near(dy, dx)).wait_send()

    own_out.wait()
    for dy, dx in PEERS:
        slot = near(dy, dx)
        o_copy(tp, slot).wait_send()
        o_copy(slot, slot).wait_recv()


def per_device(queries, keys, values, block_order):
    rows, width = queries.shape
    part = width // 8
    hbm = pl.BlockSpec(memory_space=pl.ANY)
    window = PREV + 1
    dma = pltpu.SemaphoreType.DMA
    return pl.pallas_call(
        functools.partial(kernel, block_order.shape[0]),
        out_shape=jax.ShapeDtypeStruct(queries.shape, jnp.bfloat16),
        in_specs=[hbm, hbm, hbm, hbm],
        out_specs=hbm,
        scratch_shapes=[
            pltpu.SMEM(block_order.shape, jnp.int32),
            pltpu.VMEM((8, rows, part), jnp.bfloat16),
            pltpu.VMEM((window, 8, 2, rows, HD), jnp.bfloat16),
            pltpu.VMEM((8, 2, rows, HD), jnp.bfloat16),
            pltpu.VMEM((window, 8 * rows, 2 * HD), jnp.bfloat16),
            pltpu.VMEM((8, rows, part), jnp.bfloat16),
            pltpu.SemaphoreType.REGULAR, dma, dma((2,)), dma((8, 2)), dma, dma,
            dma((3, 8)), dma((window, 8)), dma((2, 8)),
            dma((8,)), dma((8,)), dma((8,)), dma((8,)),
        ],
        compiler_params=pltpu.CompilerParams(
            collective_id=0, has_side_effects=True, vmem_limit_bytes=50331648
        ),
    )(*[pltpu.with_memory_space_constraint(a, pltpu.HBM) for a in (queries, keys, values, block_order)])


def solution(mesh):
    return jax.shard_map(
        per_device,
        mesh=mesh,
        in_specs=(P(("ctx", "tp"), None), P(("ctx", "tp"), None), P(("ctx", "tp"), None), P()),
        out_specs=P(("ctx", "tp"), None),
        check_vma=False,
    )
```

```python
import functools
import math

import jax
import jax.numpy as jnp
from jax import lax
from jax.experimental import pallas as pl
from jax.experimental.pallas import tpu as pltpu
from jax.sharding import PartitionSpec as P

HD = 128
PREV = 3
MASKED_SCORE = -1e30
MESH = pl.DeviceIdType.MESH
ORDER = ((2, 1), (1, 0), (1, 1), (3, 0), (3, 1), (2, 0), (0, 1), (0, 0))
PEERS = ORDER[:-1]
PARTS = ((0, 1), (2, 3))


def pick(index, values):
    total = jnp.int32(0)
    for position, value in enumerate(values):
        if value:
            total = total + jnp.where(index == position, jnp.int32(value), jnp.int32(0))
    return total


def kernel(
    blocks, q_hbm, k_hbm, v_hbm, order_hbm, out_ref,
    order_ref, q_buf, kv_buf, kv_own, vext, o_buf,
    clear_sem, order_sem, own_sem, load_sem, q_own_sem, o_own_sem,
    s_ss, s_rs, r_ss, q_ss, q_rs, o_ss, o_rs,
):
    ctx = lax.axis_index("ctx")
    tp = lax.axis_index("tp")
    planes = blocks // 2
    rows = q_hbm.shape[0]
    width = q_buf.shape[2]
    group = width // HD
    w, c = lax.div(ctx, 2), lax.rem(ctx, 2)
    y, xh = lax.div(tp, 2), lax.rem(tp, 2)

    def near(dy, dx):
        return lax.rem(y + dy, 4) * 2 + lax.rem(xh + dx, 2)

    def block_at(dw, core):
        return lax.rem(w + dw + planes, planes) * 2 + core

    def lanes(index, size):
        return pl.ds(pl.multiple_of(index * size, size), size)

    mate = (block_at(0, 1 - c), tp)

    loads = []
    for part, source in enumerate((k_hbm, v_hbm)):
        for h in range(8):
            loads.append(
                pltpu.make_async_copy(source.at[:, pl.ds(h * HD, HD)], kv_own.at[h, part], load_sem.at[h, part])
            )
    own_kv = [
        pltpu.make_async_copy(source.at[:, lanes(tp, HD)], kv_buf.at[0, tp, part], own_sem.at[part])
        for part, source in enumerate((k_hbm, v_hbm))
    ]
    own_q = pltpu.make_async_copy(q_hbm.at[:, lanes(tp, width)], q_buf.at[tp], q_own_sem)
    order_load = pltpu.make_async_copy(order_hbm, order_ref, order_sem)
    for copy in (*loads, *own_kv, own_q, order_load):
        copy.start()

    barrier = pltpu.get_barrier_semaphore()

    def greet(block, slot):
        pl.semaphore_signal(barrier, inc=1, device_id=(block, slot), device_id_type=MESH)

    for dy, dx in ORDER:
        greet(block_at(-1, c), near(dy, dx))

    @pl.when(c == 0)
    def _():
        greet(block_at(-1, 1), tp)

    last = lax.rem(w, planes // 2) == planes // 2 - 1

    @pl.when(jnp.logical_not(last))
    def _():
        for dy, dx in PEERS:
            greet(ctx, near(dy, dx))

    greet(*mate)
    pl.semaphore_wait(barrier, jnp.where(last, 9 + c, 16 + c))

    @pl.when(lax.rem(w + 1, planes // 2) == planes // 2 - 1)
    def _():
        pl.semaphore_signal(clear_sem, inc=1, device_id=(block_at(1, c), tp), device_id_type=MESH)

    def slice_copy(dw, slot):
        return pltpu.make_async_remote_copy(
            src_ref=kv_own.at[slot],
            dst_ref=kv_buf.at[2 * dw, tp],
            send_sem=s_ss.at[dw, slot],
            recv_sem=s_rs.at[2 * dw, tp],
            device_id=(block_at(dw, c), slot),
            device_id_type=MESH,
        )

    def onward(slot):
        return pltpu.make_async_remote_copy(
            src_ref=kv_buf.at[2, slot],
            dst_ref=kv_buf.at[3, slot],
            send_sem=s_ss.at[2, slot],
            recv_sem=s_rs.at[3, slot],
            device_id=(block_at(1, 0), tp),
            device_id_type=MESH,
        )

    def relay(offset, landing, slot):
        return pltpu.make_async_remote_copy(
            src_ref=kv_buf.at[offset, slot],
            dst_ref=kv_buf.at[landing, slot],
            send_sem=r_ss.at[offset // 2, slot],
            recv_sem=s_rs.at[landing, slot],
            device_id=mate,
            device_id_type=MESH,
        )

    def arrived(offset, slot):
        relay(0, offset, slot).wait_recv()

    def q_copy(origin, slot):
        return pltpu.make_async_remote_copy(
            src_ref=q_hbm.at[:, lanes(slot, width)],
            dst_ref=q_buf.at[origin],
            send_sem=q_ss.at[slot],
            recv_sem=q_rs.at[origin],
            device_id=(ctx, slot),
            device_id_type=MESH,
        )

    def o_copy(origin, slot):
        return pltpu.make_async_remote_copy(
            src_ref=o_buf.at[slot],
            dst_ref=out_ref.at[:, lanes(origin, width)],
            send_sem=o_ss.at[slot],
            recv_sem=o_rs.at[origin],
            device_id=(ctx, slot),
            device_id_type=MESH,
        )

    for copy in loads:
        copy.wait()
    for dy, dx in ORDER:
        slice_copy(1, near(dy, dx)).start()

    @pl.when(last)
    def _():
        pl.semaphore_wait(clear_sem, 1)

    for dy, dx in PEERS:
        slice_copy(0, near(dy, dx)).start()
    for dy, dx in PEERS:
        q_copy(tp, near(dy, dx)).start()

    for copy in own_kv:
        copy.wait()
    for dy, dx in reversed(PEERS):
        arrived(0, near(dy, dx))

        @pl.when(c == 0)
        def _(slot=near(dy, dx)):
            relay(0, 1, slot).start()

    @pl.when(c == 0)
    def _():
        relay(0, 1, tp).start()

    for dy, dx in reversed(ORDER):
        arrived(2, near(dy, dx))

        @pl.when(c == 0)
        def _(slot=near(dy, dx)):
            relay(2, 3, slot).start()

        @pl.when(c == 1)
        def _(slot=near(dy, dx)):
            onward(slot).start()
            relay(2, 1, slot).start()

    vext[:, :, HD:] = jnp.ones((PREV + 1, 8 * rows, HD), jnp.bfloat16)
    for offset in (0, 2, 1, 3):
        if offset % 2:
            for slot in range(8):
                arrived(offset, slot)
        vext[offset, :, :HD] = kv_buf[offset, :, 1].reshape(8 * rows, HD)
    own_q.wait()
    order_load.wait()

    span = 4 * rows
    factor = math.log2(math.e) / math.sqrt(HD)

    here = order_ref[ctx]
    there = [order_ref[lax.rem(ctx + blocks - step, blocks)] for step in range(1, PREV + 1)]

    def attend(slot, late):
        slots = 8 if late else 4
        count = slots * rows
        queries = jnp.concatenate([q_buf[slot, :, h * HD : (h + 1) * HD] for h in range(group)], axis=0)
        first = slot * rows - (span if late else 0)
        own_row = lax.broadcasted_iota(jnp.int32, (rows, span), 0) + first
        own_col = lax.broadcasted_iota(jnp.int32, (rows, span), 1)
        causal = jnp.where(own_col <= own_row, 0.0, MASKED_SCORE).astype(jnp.float32)
        causal = jnp.concatenate([causal] * group, axis=0)

        def scored(offsets):
            key_rows = kv_buf[offsets[0] : offsets[-1] + 1, :slots, 0].reshape(len(offsets) * count, HD)
            scores = lax.dot_general(
                queries, key_rows, (((1,), (1,)), ((), ())), preferred_element_type=jnp.float32
            )
            pieces = []
            for position, offset in enumerate(offsets):
                for half in range(slots // 4):
                    start = position * count + half * span
                    piece = scores[:, start : start + span]
                    if half == (1 if late else 0):
                        if offset == 0:
                            piece = piece + causal
                        else:
                            seen = there[offset - 1] > here if late else there[offset - 1] < here
                            piece = piece + jnp.where(seen, 0.0, MASKED_SCORE).astype(jnp.float32)
                    pieces.append(piece)
            return pieces

        total, top = None, None
        parts = [scored(offsets) for offsets in PARTS]
        for offsets, pieces in zip(PARTS, parts):
            best = jnp.max(functools.reduce(jnp.maximum, pieces), axis=1, keepdims=True)
            if top is not None:
                best = jnp.maximum(best, top)
            weights = jnp.concatenate(
                [jnp.exp2((piece - best) * factor).astype(jnp.bfloat16) for piece in pieces], axis=1
            )
            sums = jnp.dot(
                weights,
                vext[offsets[0] : offsets[-1] + 1, :count].reshape(len(offsets) * count, 2 * HD),
                preferred_element_type=jnp.float32,
            )
            total = sums if total is None else total * jnp.exp2((top - best) * factor) + sums
            top = best
        result = (total[:, :HD] / total[:, HD:]).astype(jnp.bfloat16)
        for h in range(group):
            o_buf[slot, :, h * HD : (h + 1) * HD] = result[h * rows : (h + 1) * rows]

    own_out = pltpu.make_async_copy(o_buf.at[tp], out_ref.at[:, lanes(tp, width)], o_own_sem)

    def serve(turn, carry):
        slot = near(pick(turn, [dy for dy, _ in ORDER]), pick(turn, [dx for _, dx in ORDER]))

        @pl.when(turn < len(PEERS))
        def _():
            q_copy(slot, slot).wait_recv()

        @pl.when(slot < 4)
        def _():
            attend(slot, False)

        @pl.when(slot >= 4)
        def _():
            attend(slot, True)

        @pl.when(turn < len(PEERS))
        def _():
            o_copy(tp, slot).start()

        return carry

    lax.fori_loop(0, len(ORDER), serve, 0)
    own_out.start()

    for dy, dx in PEERS:
        slot = near(dy, dx)
        q_copy(tp, slot).wait_send()
        slice_copy(0, slot).wait_send()
    for dy, dx in ORDER:
        slot = near(dy, dx)
        slice_copy(1, slot).wait_send()
        relay(2, 1, slot).wait_send()

    @pl.when(c == 0)
    def _():
        for dy, dx in ORDER:
            relay(0, 1, near(dy, dx)).wait_send()

    @pl.when(c == 1)
    def _():
        for dy, dx in ORDER:
            onward(near(dy, dx)).wait_send()

    own_out.wait()
    for dy, dx in PEERS:
        slot = near(dy, dx)
        o_copy(tp, slot).wait_send()
        o_copy(slot, slot).wait_recv()


def per_device(queries, keys, values, block_order):
    rows, width = queries.shape
    part = width // 8
    hbm = pl.BlockSpec(memory_space=pl.ANY)
    window = PREV + 1
    dma = pltpu.SemaphoreType.DMA
    return pl.pallas_call(
        functools.partial(kernel, block_order.shape[0]),
        out_shape=jax.ShapeDtypeStruct(queries.shape, jnp.bfloat16),
        in_specs=[hbm, hbm, hbm, hbm],
        out_specs=hbm,
        scratch_shapes=[
            pltpu.SMEM(block_order.shape, jnp.int32),
            pltpu.VMEM((8, rows, part), jnp.bfloat16),
            pltpu.VMEM((window, 8, 2, rows, HD), jnp.bfloat16),
            pltpu.VMEM((8, 2, rows, HD), jnp.bfloat16),
            pltpu.VMEM((window, 8 * rows, 2 * HD), jnp.bfloat16),
            pltpu.VMEM((8, rows, part), jnp.bfloat16),
            pltpu.SemaphoreType.REGULAR, dma, dma((2,)), dma((8, 2)), dma, dma,
            dma((3, 8)), dma((window, 8)), dma((2, 8)),
            dma((8,)), dma((8,)), dma((8,)), dma((8,)),
        ],
        compiler_params=pltpu.CompilerParams(
            collective_id=0, has_side_effects=True, vmem_limit_bytes=50331648
        ),
    )(*[pltpu.with_memory_space_constraint(a, pltpu.HBM) for a in (queries, keys, values, block_order)])


def solution(mesh):
    return jax.shard_map(
        per_device,
        mesh=mesh,
        in_specs=(P(("ctx", "tp"), None), P(("ctx", "tp"), None), P(("ctx", "tp"), None), P()),
        out_specs=P(("ctx", "tp"), None),
        check_vma=False,
    )
```

```python
import functools
import math

import jax
import jax.numpy as jnp
from jax import lax
from jax.experimental import pallas as pl
from jax.experimental.pallas import tpu as pltpu
from jax.sharding import PartitionSpec as P

HD = 128
PREV = 3
MASKED_SCORE = -1e30
MESH = pl.DeviceIdType.MESH
ORDER = ((2, 1), (1, 1), (3, 1), (2, 0), (0, 1), (1, 0), (3, 0), (0, 0))
PEERS = ORDER[:-1]
PARTS = ((0, 1), (2, 3))


def pick(index, values):
    total = jnp.int32(0)
    for position, value in enumerate(values):
        if value:
            total = total + jnp.where(index == position, jnp.int32(value), jnp.int32(0))
    return total


def kernel(
    blocks, q_hbm, k_hbm, v_hbm, order_hbm, out_ref,
    order_ref, q_buf, kv_buf, kv_own, vext, o_buf,
    clear_sem, order_sem, own_sem, load_sem, q_own_sem, o_own_sem,
    s_ss, s_rs, r_ss, q_ss, q_rs, o_ss, o_rs,
):
    ctx = lax.axis_index("ctx")
    tp = lax.axis_index("tp")
    planes = blocks // 2
    rows = q_hbm.shape[0]
    width = q_buf.shape[2]
    group = width // HD
    w, c = lax.div(ctx, 2), lax.rem(ctx, 2)
    y, xh = lax.div(tp, 2), lax.rem(tp, 2)

    def near(dy, dx):
        return lax.rem(y + dy, 4) * 2 + lax.rem(xh + dx, 2)

    def block_at(dw, core):
        return lax.rem(w + dw + planes, planes) * 2 + core

    def lanes(index, size):
        return pl.ds(pl.multiple_of(index * size, size), size)

    mate = (block_at(0, 1 - c), tp)

    loads = []
    for part, source in enumerate((k_hbm, v_hbm)):
        for h in range(8):
            loads.append(
                pltpu.make_async_copy(source.at[:, pl.ds(h * HD, HD)], kv_own.at[h, part], load_sem.at[h, part])
            )
    own_kv = [
        pltpu.make_async_copy(source.at[:, lanes(tp, HD)], kv_buf.at[0, tp, part], own_sem.at[part])
        for part, source in enumerate((k_hbm, v_hbm))
    ]
    own_q = pltpu.make_async_copy(q_hbm.at[:, lanes(tp, width)], q_buf.at[tp], q_own_sem)
    order_load = pltpu.make_async_copy(order_hbm, order_ref, order_sem)
    for copy in loads:
        copy.start()

    barrier = pltpu.get_barrier_semaphore()

    def greet(block, slot):
        pl.semaphore_signal(barrier, inc=1, device_id=(block, slot), device_id_type=MESH)

    for dy, dx in ORDER:
        greet(block_at(-1, c), near(dy, dx))

    @pl.when(c == 0)
    def _():
        greet(block_at(-1, 1), tp)

    last = lax.rem(w, planes // 2) == planes // 2 - 1

    @pl.when(jnp.logical_not(last))
    def _():
        for dy, dx in PEERS:
            greet(ctx, near(dy, dx))

    greet(*mate)
    for copy in (*own_kv, own_q, order_load):
        copy.start()
    pl.semaphore_wait(barrier, jnp.where(last, 9 + c, 16 + c))

    @pl.when(lax.rem(w + 1, planes // 2) == planes // 2 - 1)
    def _():
        pl.semaphore_signal(clear_sem, inc=1, device_id=(block_at(1, c), tp), device_id_type=MESH)

    def slice_copy(dw, slot):
        return pltpu.make_async_remote_copy(
            src_ref=kv_own.at[slot],
            dst_ref=kv_buf.at[2 * dw, tp],
            send_sem=s_ss.at[dw, slot],
            recv_sem=s_rs.at[2 * dw, tp],
            device_id=(block_at(dw, c), slot),
            device_id_type=MESH,
        )

    def onward(slot):
        return pltpu.make_async_remote_copy(
            src_ref=kv_buf.at[2, slot],
            dst_ref=kv_buf.at[3, slot],
            send_sem=s_ss.at[2, slot],
            recv_sem=s_rs.at[3, slot],
            device_id=(block_at(1, 0), tp),
            device_id_type=MESH,
        )

    def relay(offset, landing, slot):
        return pltpu.make_async_remote_copy(
            src_ref=kv_buf.at[offset, slot],
            dst_ref=kv_buf.at[landing, slot],
            send_sem=r_ss.at[offset // 2, slot],
            recv_sem=s_rs.at[landing, slot],
            device_id=mate,
            device_id_type=MESH,
        )

    def arrived(offset, slot):
        relay(0, offset, slot).wait_recv()

    def q_copy(origin, slot):
        return pltpu.make_async_remote_copy(
            src_ref=q_hbm.at[:, lanes(slot, width)],
            dst_ref=q_buf.at[origin],
            send_sem=q_ss.at[slot],
            recv_sem=q_rs.at[origin],
            device_id=(ctx, slot),
            device_id_type=MESH,
        )

    def o_copy(origin, slot):
        return pltpu.make_async_remote_copy(
            src_ref=o_buf.at[slot],
            dst_ref=out_ref.at[:, lanes(origin, width)],
            send_sem=o_ss.at[slot],
            recv_sem=o_rs.at[origin],
            device_id=(ctx, slot),
            device_id_type=MESH,
        )

    for copy in loads:
        copy.wait()
    for dy, dx in ORDER:
        slice_copy(1, near(dy, dx)).start()

    @pl.when(last)
    def _():
        pl.semaphore_wait(clear_sem, 1)

    for dy, dx in PEERS:
        slice_copy(0, near(dy, dx)).start()
    for dy, dx in PEERS:
        q_copy(tp, near(dy, dx)).start()

    for copy in own_kv:
        copy.wait()
    for dy, dx in reversed(PEERS):
        arrived(0, near(dy, dx))

        @pl.when(c == 0)
        def _(slot=near(dy, dx)):
            relay(0, 1, slot).start()

    @pl.when(c == 0)
    def _():
        relay(0, 1, tp).start()

    for dy, dx in reversed(ORDER):
        arrived(2, near(dy, dx))

        @pl.when(c == 0)
        def _(slot=near(dy, dx)):
            relay(2, 3, slot).start()

        @pl.when(c == 1)
        def _(slot=near(dy, dx)):
            onward(slot).start()
            relay(2, 1, slot).start()

    vext[:, :, HD:] = jnp.ones((PREV + 1, 8 * rows, HD), jnp.bfloat16)
    for offset in (0, 2, 1, 3):
        if offset % 2:
            for slot in range(8):
                arrived(offset, slot)
        vext[offset, :, :HD] = kv_buf[offset, :, 1].reshape(8 * rows, HD)
    own_q.wait()
    order_load.wait()

    span = 4 * rows
    factor = math.log2(math.e) / math.sqrt(HD)

    here = order_ref[ctx]
    there = [order_ref[lax.rem(ctx + blocks - step, blocks)] for step in range(1, PREV + 1)]

    def attend(slot, late):
        slots = 8 if late else 4
        count = slots * rows
        queries = jnp.concatenate([q_buf[slot, :, h * HD : (h + 1) * HD] for h in range(group)], axis=0)
        first = slot * rows - (span if late else 0)
        own_row = lax.broadcasted_iota(jnp.int32, (rows, span), 0) + first
        own_col = lax.broadcasted_iota(jnp.int32, (rows, span), 1)
        causal = jnp.where(own_col <= own_row, 0.0, MASKED_SCORE).astype(jnp.float32)
        causal = jnp.concatenate([causal] * group, axis=0)

        def scored(offsets):
            key_rows = kv_buf[offsets[0] : offsets[-1] + 1, :slots, 0].reshape(len(offsets) * count, HD)
            scores = lax.dot_general(
                queries, key_rows, (((1,), (1,)), ((), ())), preferred_element_type=jnp.float32
            )
            pieces = []
            for position, offset in enumerate(offsets):
                for half in range(slots // 4):
                    start = position * count + half * span
                    piece = scores[:, start : start + span]
                    if half == (1 if late else 0):
                        if offset == 0:
                            piece = piece + causal
                        else:
                            seen = there[offset - 1] > here if late else there[offset - 1] < here
                            piece = piece + jnp.where(seen, 0.0, MASKED_SCORE).astype(jnp.float32)
                    pieces.append(piece)
            return pieces

        total, top = None, None
        parts = [scored(offsets) for offsets in PARTS]
        for offsets, pieces in zip(PARTS, parts):
            best = jnp.max(functools.reduce(jnp.maximum, pieces), axis=1, keepdims=True)
            if top is not None:
                best = jnp.maximum(best, top)
            weights = jnp.concatenate(
                [jnp.exp2((piece - best) * factor).astype(jnp.bfloat16) for piece in pieces], axis=1
            )
            sums = jnp.dot(
                weights,
                vext[offsets[0] : offsets[-1] + 1, :count].reshape(len(offsets) * count, 2 * HD),
                preferred_element_type=jnp.float32,
            )
            total = sums if total is None else total * jnp.exp2((top - best) * factor) + sums
            top = best
        result = (total[:, :HD] / total[:, HD:]).astype(jnp.bfloat16)
        for h in range(group):
            o_buf[slot, :, h * HD : (h + 1) * HD] = result[h * rows : (h + 1) * rows]

    own_out = pltpu.make_async_copy(o_buf.at[tp], out_ref.at[:, lanes(tp, width)], o_own_sem)

    def serve(turn, carry):
        slot = near(pick(turn, [dy for dy, _ in ORDER]), pick(turn, [dx for _, dx in ORDER]))

        @pl.when(turn < len(PEERS))
        def _():
            q_copy(slot, slot).wait_recv()

        @pl.when(slot < 4)
        def _():
            attend(slot, False)

        @pl.when(slot >= 4)
        def _():
            attend(slot, True)

        @pl.when(turn < len(PEERS))
        def _():
            o_copy(tp, slot).start()

        return carry

    lax.fori_loop(0, len(ORDER), serve, 0)
    own_out.start()

    for dy, dx in PEERS:
        slot = near(dy, dx)
        q_copy(tp, slot).wait_send()
        slice_copy(0, slot).wait_send()
    for dy, dx in ORDER:
        slot = near(dy, dx)
        slice_copy(1, slot).wait_send()
        relay(2, 1, slot).wait_send()

    @pl.when(c == 0)
    def _():
        for dy, dx in ORDER:
            relay(0, 1, near(dy, dx)).wait_send()

    @pl.when(c == 1)
    def _():
        for dy, dx in ORDER:
            onward(near(dy, dx)).wait_send()

    own_out.wait()
    for dy, dx in PEERS:
        slot = near(dy, dx)
        o_copy(tp, slot).wait_send()
        o_copy(slot, slot).wait_recv()


def per_device(queries, keys, values, block_order):
    rows, width = queries.shape
    part = width // 8
    hbm = pl.BlockSpec(memory_space=pl.ANY)
    window = PREV + 1
    dma = pltpu.SemaphoreType.DMA
    return pl.pallas_call(
        functools.partial(kernel, block_order.shape[0]),
        out_shape=jax.ShapeDtypeStruct(queries.shape, jnp.bfloat16),
        in_specs=[hbm, hbm, hbm, hbm],
        out_specs=hbm,
        scratch_shapes=[
            pltpu.SMEM(block_order.shape, jnp.int32),
            pltpu.VMEM((8, rows, part), jnp.bfloat16),
            pltpu.VMEM((window, 8, 2, rows, HD), jnp.bfloat16),
            pltpu.VMEM((8, 2, rows, HD), jnp.bfloat16),
            pltpu.VMEM((window, 8 * rows, 2 * HD), jnp.bfloat16),
            pltpu.VMEM((8, rows, part), jnp.bfloat16),
            pltpu.SemaphoreType.REGULAR, dma, dma((2,)), dma((8, 2)), dma, dma,
            dma((3, 8)), dma((window, 8)), dma((2, 8)),
            dma((8,)), dma((8,)), dma((8,)), dma((8,)),
        ],
        compiler_params=pltpu.CompilerParams(
            collective_id=0, has_side_effects=True, vmem_limit_bytes=50331648
        ),
    )(*[pltpu.with_memory_space_constraint(a, pltpu.HBM) for a in (queries, keys, values, block_order)])


def solution(mesh):
    return jax.shard_map(
        per_device,
        mesh=mesh,
        in_specs=(P(("ctx", "tp"), None), P(("ctx", "tp"), None), P(("ctx", "tp"), None), P()),
        out_specs=P(("ctx", "tp"), None),
        check_vma=False,
    )
```
